32 devices in a mesh: seq: 8 (over z, y), head: 4 (over x, core).
Axes of the slice: x: 2, y: 2, z: 4, core: 2. Of those that a mesh axis runs over, the one named last changes fastest.
Arguments:
- x_raw: bfloat16 [8192, 5120], P('seq', 'head'), may hold values from -6 to 6
- bc_raw: bfloat16 [8192, 256], P('seq'), may hold values from -6 to 6
- z_gate: bfloat16 [8192, 5120], P('seq', 'head'), may hold values from -6 to 6
- dt_raw: float32 [80, 8192], P('head', 'seq'), may hold values from -5.5 to 2.5
- a_log: float32 [80], P('head'), may hold values from -12 to -2
- d_skip: float32 [80], P('head'), may hold values from 0.5 to 1.5
- conv_x: float32 [4, 5120], P(None, 'head'), may hold values from -3 to 3
- conv_bc: float32 [4, 256], replicated, may hold values from -3 to 3
- norm_gain: float32 [5120], P('head'), may hold values from 0.1 to 1.9
- w_out: bfloat16 [5120, 2560], P('head'), may hold values from -0.125 to 0.125
Outputs:
- layer_out: bfloat16 [8192, 2560], P('seq', 'head')
The draws below stay inside these ranges and needn't reach their ends.
All inputs are finite; a program needn't handle non-finite values.
Results may differ from the reference program's by a relative error of at most 0.015.
Values may be sent and summed in bfloat16 or wider, within the bound.
A program may use at most 128 MiB of HBM per device.

```python
import jax
import jax.numpy as jnp
from jax import lax

D = 2560
H = 80
P_SIZE = 64
N = 128
Q = 256
CONV = 4
TOKENS = 8192
N_HEAD = 4


def slow_heads(key):
    share = 0.5
    return jax.random.uniform(jax.random.fold_in(key, 11), (H,)) < share


def draw_a_log(key, part):
    slow = slow_heads(key)
    picked = jax.random.uniform(jax.random.fold_in(key, 12), (H,), jnp.float32)
    slow_base = jnp.minimum(jnp.log(30.0 / TOKENS), -2.05)
    slow_rate = slow_base + picked * jnp.log(0.1)
    fast_rate = jnp.log(0.03) + picked * (jnp.log(0.08) - jnp.log(0.03))
    return jnp.where(slow, slow_rate, fast_rate).astype(jnp.float32)


def draw_dt_raw(key, part):
    slow = slow_heads(key)
    noise = 0.5 * jax.random.truncated_normal(jax.random.fold_in(key, 13), -3.0, 3.0, (H, TOKENS), jnp.float32)
    offsets = jax.random.uniform(jax.random.fold_in(key, 14), (H, TOKENS // Q), jnp.float32, -1.0, 1.0)
    shifted = noise + jnp.repeat(offsets, Q, axis=1)
    return (shifted + jnp.where(slow, -3.0, 0.0)[:, None]).astype(jnp.float32)


def spiked(result, key, source, target, parts, factor):
    owner, partner = [(jnp.arange(result.shape[dim]) // (result.shape[dim] // parts)).reshape([-1 if axis == dim else 1 for axis in range(result.ndim)]) for dim in (source, target)]
    chosen = jax.random.permutation(key, parts)[partner]
    strong = (owner == chosen) | (owner == (partner + parts // 2) % parts)
    return jnp.where(strong, factor * result, result)


def block_scale(stream_key, dims, cuts, low, top_value):
    gain, own = 1.0, jax.random.fold_in(stream_key, 6)
    for position, parts in cuts:
        steps = jnp.exp(jax.random.uniform(jax.random.fold_in(own, position), (parts,), jnp.float32, low / len(cuts), top_value / len(cuts)))
        gain = gain * jnp.repeat(steps, dims[position] // parts).reshape([-1 if axis == position else 1 for axis in range(len(dims))])
    return gain


def gaussian(rng, shape, width, most, split=(), kind=jnp.bfloat16):
    level = block_scale(rng, shape, split, -0.22, 0.18) if split else 1.0
    array = jax.random.normal(rng, shape, jnp.float32) * width * level
    return jnp.minimum(jnp.maximum(array, -most), most).astype(kind)


def noise_with(stream_key, shape, width, reach, shards, heavy, held_as=jnp.bfloat16):
    result = width * jax.random.normal(stream_key, shape, jnp.float32)
    if shards:
        result = result * block_scale(stream_key, shape, shards, -0.22, 0.18)
    return jnp.clip(spiked(result, jax.random.fold_in(stream_key, 3), *heavy), -reach, reach).astype(held_as)


def setup_inputs(seed: int = 0) -> dict:
    keys = jax.random.split(jax.random.key(seed), 11)
    x_raw = gaussian(keys[0], (TOKENS, H * P_SIZE), 1.0, 6.0, ((0, 8), (1, 4)))
    bc_raw = gaussian(keys[1], (TOKENS, 2 * N), 1.0, 6.0, ((0, 8),))
    z_gate = gaussian(keys[2], (TOKENS, H * P_SIZE), 1.0, 6.0, ((0, 8), (1, 4)))
    dt_raw = draw_dt_raw(jax.random.fold_in(keys[10], 71), 0)
    a_log = draw_a_log(jax.random.fold_in(keys[10], 71), 0)
    d_skip = jnp.clip(0.5 + 1.0 * jax.random.uniform(keys[5], (H,), jnp.float32) ** block_scale(keys[5], (H,), ((0, 4),), -0.2, 0.2), 0.5, 1.5)
    conv_x = gaussian(keys[6], (CONV, H * P_SIZE), CONV ** -0.5, 3.0, ((1, 4),), jnp.float32)
    conv_bc = gaussian(keys[7], (CONV, 2 * N), CONV ** -0.5, 3.0, (), jnp.float32)
    norm_gain = jnp.clip(1.0 + 0.18 * jax.random.normal(keys[8], (H * P_SIZE,), jnp.float32), 0.1, 1.9)
    w_out = noise_with(keys[9], (H * P_SIZE, D), (H * P_SIZE) ** -0.5, 0.125, ((0, 4),), (0, 1, 4, 2.0))
    return dict(x_raw=x_raw, bc_raw=bc_raw, z_gate=z_gate, dt_raw=dt_raw, a_log=a_log, d_skip=d_skip, conv_x=conv_x, conv_bc=conv_bc, norm_gain=norm_gain, w_out=w_out)


norm_floor = 0.5

def causal_conv(raw_rows, taps):
    length = raw_rows.shape[0]
    padded = jnp.concatenate([jnp.zeros((CONV - 1, raw_rows.shape[1]), jnp.bfloat16), raw_rows], axis=0)
    total = jnp.zeros(raw_rows.shape, jnp.float32)
    for number in range(CONV):
        total = total + padded[number:number + length].astype(jnp.float32) * taps[number][None, :]
    return jax.nn.silu(total).astype(jnp.bfloat16)

def reference(x_raw, bc_raw, z_gate, dt_raw, a_log, d_skip, conv_x, conv_bc, norm_gain, w_out):
    x_conv = causal_conv(x_raw, conv_x)
    bc_conv = causal_conv(bc_raw, conv_bc)
    block_count = TOKENS // Q
    x_heads = x_conv.reshape(block_count, Q, H, P_SIZE)
    b_part = bc_conv[:, :N].reshape(block_count, Q, N)
    c_part = bc_conv[:, N:].reshape(block_count, Q, N)
    step_sizes = jax.nn.softplus(dt_raw)
    log_rates = -jnp.exp(a_log)[:, None] * step_sizes
    rates_blocks = log_rates.reshape(H, block_count, Q).transpose(1, 0, 2)
    steps_blocks = step_sizes.reshape(H, block_count, Q).transpose(1, 0, 2)
    causal = jnp.tril(jnp.ones((Q, Q), bool))

    def block_step(carried, inputs):
        x_block, b_block, c_block, rate_block, step_block = inputs
        cumulative = jnp.cumsum(rate_block, axis=1)
        scores = jnp.dot(c_block, b_block.T, preferred_element_type=jnp.float32)
        log_gaps = cumulative[:, :, None] - cumulative[:, None, :]
        decays = jnp.where(causal[None], jnp.exp(jnp.where(causal[None], log_gaps, 0.0)), 0.0)
        weights = (scores[None] * decays * step_block[:, None, :]).astype(jnp.bfloat16)
        x_float = x_block.astype(jnp.float32)
        inner_out = jnp.einsum('hts,shp->thp', weights.astype(jnp.float32), x_float)
        outer_out = jnp.einsum('tn,hpn->thp', c_block.astype(jnp.float32), carried, precision=lax.Precision.HIGHEST) * jnp.exp(cumulative).T[:, :, None]
        tail_decay = jnp.exp(cumulative[:, -1:] - cumulative) * step_block
        weighted_b = (b_block.astype(jnp.float32)[None] * tail_decay[:, :, None]).astype(jnp.bfloat16)
        local_states = jnp.einsum('hsn,shp->hpn', weighted_b.astype(jnp.float32), x_float)
        updated = jnp.exp(cumulative[:, -1])[:, None, None] * carried + local_states
        mixed = inner_out + outer_out + d_skip[None, :, None] * x_float
        return (updated, mixed)
    start_state = jnp.zeros((H, P_SIZE, N), jnp.float32)
    _, mixed_all = lax.scan(block_step, start_state, (x_heads, b_part, c_part, rates_blocks, steps_blocks))
    mixed_all = mixed_all.reshape(TOKENS, H * P_SIZE)
    gated = mixed_all * jax.nn.silu(z_gate.astype(jnp.float32))
    mean_square = lax.optimization_barrier(jnp.sum(gated * gated, axis=1)) / (H * P_SIZE) + norm_floor
    unit = (gated * norm_gain[None, :]).astype(jnp.bfloat16)
    group_width = H * P_SIZE // N_HEAD
    summed = jnp.zeros((TOKENS, D), jnp.float32)
    for group in range(N_HEAD):
        columns = unit[:, group * group_width:(group + 1) * group_width]
        rows_out = w_out[group * group_width:(group + 1) * group_width]
        group_part = jnp.dot(columns, rows_out, preferred_element_type=jnp.float32).astype(jnp.bfloat16)
        summed = summed + group_part.astype(jnp.float32)
    return (summed * lax.rsqrt(mean_square)[:, None]).astype(jnp.bfloat16)
```

```python
import functools

import jax
import jax.numpy as jnp
import numpy as np
from jax import lax
from jax.experimental import pallas as pl
from jax.experimental.pallas import tpu as pltpu
from jax.sharding import PartitionSpec as P

P_SIZE = 64
N = 128
Q = 256
CONV = 4
RIM = 16
CHUNK = 256
SLOT = 32

norm_floor = 0.5


def passed_along(value, axis, steps):
    count = lax.axis_size(axis)
    initial, last = (max(0, -steps), min(count, count - steps))
    return lax.ppermute(value, axis, [(source, source + steps) for source in range(initial, last)])


def silu(v):
    return v / (1.0 + jnp.exp(-v))


def dot_t(a, b):
    return lax.dot_general(a, b, (((0,), (0,)), ((), ())), preferred_element_type=jnp.float32)


def conv_rows(padded_ref, taps, cols, rows):
    total = padded_ref[pl.ds(RIM - CONV + 1, rows), cols] * taps[0:1]
    for number in range(1, CONV):
        total = total + padded_ref[pl.ds(RIM - CONV + 1 + number, rows), cols] * taps[number : number + 1]
    return silu(total)


def store_split(ref, at, value, heads):
    high = value.astype(jnp.bfloat16)
    low = (value - high.astype(jnp.float32)).astype(jnp.bfloat16)
    width = value.shape[1]
    ref[0:heads, at : at + width] = high
    ref[SLOT : SLOT + heads, at : at + width] = low


def intra_kernel(
    heads, width,
    x_ref, xprev_ref, bc_ref, bcprev_ref, before_ref, dt_ref, a_ref, d_ref, cx_ref, cbc_ref, spread_ref, tri_ref,
    base_ref, c_ref, fac2_ref, state_ref, log_ref,
    xpad, bcpad, fac, run, plog, bt, masked,
):
    block = pl.program_id(0)

    @pl.when(block == 0)
    def _():
        run[...] = jnp.zeros_like(run)
        plog[...] = jnp.zeros_like(plog)
        fac[...] = jnp.zeros_like(fac)
        xpad[0:RIM, :] = before_ref[:, 0:width].astype(jnp.float32)
        bcpad[0:RIM, :] = before_ref[:, width : width + 2 * N].astype(jnp.float32)

    @pl.when(block > 0)
    def _():
        xpad[0:RIM, :] = xprev_ref[...].astype(jnp.float32)
        bcpad[0:RIM, :] = bcprev_ref[...].astype(jnp.float32)

    xpad[RIM : RIM + Q, :] = x_ref[...].astype(jnp.float32)
    bcpad[RIM : RIM + Q, :] = bc_ref[...].astype(jnp.float32)
    bc = conv_rows(bcpad, cbc_ref[...], slice(None), Q)
    b_part = bc[:, :N].astype(jnp.bfloat16)
    c_part = bc[:, N:].astype(jnp.bfloat16)
    c_ref[...] = c_part
    bt[...] = bc[:, :N].T.astype(jnp.bfloat16)
    scores = lax.dot_general(c_part, b_part, (((1,), (1,)), ((), ())), preferred_element_type=jnp.float32)
    rows_at = lax.broadcasted_iota(jnp.int32, (Q, Q), 0)
    cols_at = lax.broadcasted_iota(jnp.int32, (Q, Q), 1)
    masked[...] = jnp.where(rows_at >= cols_at, scores, 0.0).astype(jnp.bfloat16)

    dt = dt_ref[...]
    step = jnp.maximum(dt, 0.0) + jnp.log1p(jnp.exp(-jnp.abs(dt)))
    rate = -jnp.exp(a_ref[...]) * step
    tri = tri_ref[...]
    cum = jnp.zeros_like(rate)
    rest = rate
    for _ in range(3):
        piece = rest.astype(jnp.bfloat16)
        cum = cum + jnp.dot(piece, tri, preferred_element_type=jnp.float32)
        rest = rest - piece.astype(jnp.float32)
    last = cum[:, Q - 1 : Q]
    mid = 0.5 * last
    store_split(fac, 0, jnp.exp(cum - mid), heads)
    store_split(fac, Q, jnp.exp(mid - cum) * step, heads)
    lane = lax.broadcasted_iota(jnp.int32, (heads, 128), 1)
    scal = jnp.where(lane == 0, last, jnp.where(lane == 1, mid, last - mid))
    store_split(fac, 2 * Q, jnp.exp(scal), heads)
    before_log = plog[...][:, 0:1]
    fac2_ref[...] = jnp.zeros_like(fac2_ref)
    store_split(fac2_ref, 0, jnp.exp(before_log + cum), heads)
    plog[...] = jnp.broadcast_to(before_log + last, plog.shape)
    log_ref[...] = plog[...]

    for col in range(0, width, CHUNK):
        cols = slice(col, col + CHUNK)
        wide = dot_t(fac[...], spread_ref[:, cols])
        xc = conv_rows(xpad, cx_ref[:, cols], cols, Q).astype(jnp.bfloat16).astype(jnp.float32)
        scaled = (xc * wide[Q : 2 * Q]).astype(jnp.bfloat16)
        held = run[:, cols]
        decay = wide[2 * Q : 2 * Q + 1]
        to_mid = wide[2 * Q + 1 : 2 * Q + 2]
        from_mid = wide[2 * Q + 2 : 2 * Q + 3]
        y = jnp.dot(masked[...], scaled, preferred_element_type=jnp.float32)
        y = y + jnp.dot(c_part, (held * to_mid).astype(jnp.bfloat16), preferred_element_type=jnp.float32)
        base_ref[:, cols] = wide[0:Q] * y + d_ref[:, cols] * xc
        added = jnp.dot(bt[...], scaled, preferred_element_type=jnp.float32)
        new = held * decay + from_mid * added
        run[:, cols] = new
        state_ref[:, cols] = new.astype(jnp.bfloat16)


def project_kernel(width, base_ref, z_ref, c_ref, fac2_ref, enter_ref, gain_ref, spread_ref, w_ref, part_ref, sq_ref, unit):
    total = jnp.zeros((Q, 128), jnp.float32)
    for col in range(0, width, CHUNK):
        cols = slice(col, col + CHUNK)
        wide = dot_t(fac2_ref[...], spread_ref[:, cols])
        outer = jnp.dot(c_ref[...], enter_ref[:, cols], preferred_element_type=jnp.float32)
        mixed = base_ref[:, cols] + wide * outer
        gated = mixed * silu(z_ref[:, cols].astype(jnp.float32))
        square = gated * gated
        for part in range(0, CHUNK, 128):
            total = total + square[:, part : part + 128]
        unit[:, cols] = (gated * gain_ref[:, cols]).astype(jnp.bfloat16)
    sq_ref[...] = lax.dot_general(
        jnp.ones((8, 128), jnp.float32), total, (((1,), (1,)), ((), ())),
        precision=lax.Precision.HIGHEST, preferred_element_type=jnp.float32,
    )
    part_ref[...] = jnp.dot(unit[...], w_ref[...], preferred_element_type=jnp.float32).astype(jnp.bfloat16)


def full(shape):
    return pl.BlockSpec(shape, lambda i: (0,) * len(shape))


def local(channels, x_raw, bc_raw, z_gate, dt_raw, a_log, d_skip, conv_x, conv_bc, norm_gain, w_out):
    length, width = x_raw.shape
    heads = a_log.shape[0]
    blocks = length // Q
    depth = w_out.shape[1]
    spread = np.zeros((2 * SLOT, width), np.float32)
    for head in range(heads):
        spread[head, head * P_SIZE : (head + 1) * P_SIZE] = 1.0
        spread[SLOT + head, head * P_SIZE : (head + 1) * P_SIZE] = 1.0
    spread = jnp.asarray(spread, jnp.bfloat16)
    tri = jnp.asarray(np.triu(np.ones((Q, Q), np.float32)), jnp.bfloat16)
    rim_rows = jnp.concatenate([x_raw[length - RIM :], bc_raw[length - RIM :]], axis=1)
    before = passed_along(rim_rows, "seq", 1)
    d_wide = jnp.repeat(d_skip, P_SIZE)[None]
    prev = lambda i: (jnp.maximum(i * (Q // RIM) - 1, 0), 0)
    f32, bf16 = jnp.float32, jnp.bfloat16
    base, c_part, fac2, state, logs = pl.pallas_call(
        functools.partial(intra_kernel, heads, width),
        grid=(blocks,),
        in_specs=[
            pl.BlockSpec((Q, width), lambda i: (i, 0)),
            pl.BlockSpec((RIM, width), prev),
            pl.BlockSpec((Q, 2 * N), lambda i: (i, 0)),
            pl.BlockSpec((RIM, 2 * N), prev),
            full((RIM, width + 2 * N)),
            pl.BlockSpec((heads, Q), lambda i: (0, i)),
            full((heads, 1)),
            full((1, width)),
            full((CONV, width)),
            full((CONV, 2 * N)),
            full((2 * SLOT, width)),
            full((Q, Q)),
        ],
        out_specs=[
            pl.BlockSpec((Q, width), lambda i: (i, 0)),
            pl.BlockSpec((Q, N), lambda i: (i, 0)),
            pl.BlockSpec((2 * SLOT, Q), lambda i: (0, i)),
            full((N, width)),
            full((heads, 128)),
        ],
        out_shape=[
            jax.ShapeDtypeStruct((length, width), f32),
            jax.ShapeDtypeStruct((length, N), bf16),
            jax.ShapeDtypeStruct((2 * SLOT, length), bf16),
            jax.ShapeDtypeStruct((N, width), bf16),
            jax.ShapeDtypeStruct((heads, 128), f32),
        ],
        scratch_shapes=[
            pltpu.VMEM((RIM + Q, width), f32),
            pltpu.VMEM((RIM + Q, 2 * N), f32),
            pltpu.VMEM((2 * SLOT, 2 * Q + 128), bf16),
            pltpu.VMEM((N, width), f32),
            pltpu.VMEM((heads, 128), f32),
            pltpu.VMEM((N, Q), bf16),
            pltpu.VMEM((Q, Q), bf16),
        ],
        compiler_params=pltpu.CompilerParams(dimension_semantics=("arbitrary",)),
    )(x_raw, x_raw, bc_raw, bc_raw, before, dt_raw, a_log[:, None], d_wide, conv_x, conv_bc, spread, tri)

    own_log = logs[:, 0]
    all_logs = lax.all_gather(own_log[None], "seq", axis=0, tiled=True)
    inclusive = jnp.cumsum(all_logs, axis=0)
    own_index = lax.axis_index("seq")
    own_inclusive = lax.dynamic_index_in_dim(inclusive, own_index, 0, keepdims=False)
    before_own = own_inclusive - own_log
    piece = lax.all_gather(state[None], "seq", axis=0, tiled=True).astype(f32)
    positions = jnp.arange(piece.shape[0], dtype=jnp.int32)
    earlier = (positions < own_index)[:, None]
    exponent = jnp.where(earlier, before_own[None, :] - inclusive, 0.0)
    factors = jnp.where(earlier, jnp.exp(exponent), 0.0)
    entering = jnp.sum(piece * jnp.repeat(factors, P_SIZE, axis=1)[:, None, :], axis=0).astype(bf16)

    part, squares = pl.pallas_call(
        functools.partial(project_kernel, width),
        grid=(blocks,),
        in_specs=[
            pl.BlockSpec((Q, width), lambda i: (i, 0)),
            pl.BlockSpec((Q, width), lambda i: (i, 0)),
            pl.BlockSpec((Q, N), lambda i: (i, 0)),
            pl.BlockSpec((2 * SLOT, Q), lambda i: (0, i)),
            full((N, width)),
            full((1, width)),
            full((2 * SLOT, width)),
            full((width, depth)),
        ],
        out_specs=[pl.BlockSpec((Q, depth), lambda i: (i, 0)), pl.BlockSpec((8, Q), lambda i: (0, i))],
        out_shape=[jax.ShapeDtypeStruct((length, depth), bf16), jax.ShapeDtypeStruct((8, length), f32)],
        scratch_shapes=[pltpu.VMEM((Q, width), bf16)],
        compiler_params=pltpu.CompilerParams(dimension_semantics=("arbitrary",), vmem_limit_bytes=60 << 20),
    )(base, z_gate, c_part, fac2, entering, norm_gain[None], spread, w_out)

    row_scale = lax.rsqrt(lax.psum(squares[0], "head") / channels + norm_floor)
    summed = lax.psum_scatter(part, "head", scatter_dimension=1, tiled=True).astype(f32)
    return (summed * row_scale[:, None]).astype(bf16)


def solution(mesh):
    in_specs = (
        P("seq", "head"),
        P("seq", None),
        P("seq", "head"),
        P("head", "seq"),
        P("head"),
        P("head"),
        P(None, "head"),
        P(),
        P("head"),
        P("head", None),
    )

    def whole(x_raw, *rest):
        body = functools.partial(local, x_raw.shape[1])
        return jax.shard_map(
            body, mesh=mesh, in_specs=in_specs, out_specs=P("seq", "head"), check_vma=False
        )(x_raw, *rest)

    return whole
```

```python
import functools

import jax
import jax.numpy as jnp
import numpy as np
from jax import lax
from jax.experimental import pallas as pl
from jax.experimental.pallas import tpu as pltpu
from jax.sharding import PartitionSpec as P

P_SIZE = 64
N = 128
Q = 256
CONV = 4
RIM = 16
LANES = 128
CHUNK = 256
SLOT = 32

norm_floor = 0.5


def silu(v):
    return v / (1.0 + jnp.exp(-v))


def dot_t(a, b):
    return lax.dot_general(a, b, (((0,), (0,)), ((), ())), preferred_element_type=jnp.float32)


def conv_rows(padded_ref, taps, cols, rows):
    total = padded_ref[pl.ds(RIM - CONV + 1, rows), cols] * taps[0:1]
    for number in range(1, CONV):
        total = total + padded_ref[pl.ds(RIM - CONV + 1 + number, rows), cols] * taps[number : number + 1]
    return silu(total)


def store_split(ref, at, value, heads):
    high = value.astype(jnp.bfloat16)
    low = (value - high.astype(jnp.float32)).astype(jnp.bfloat16)
    width = value.shape[1]
    ref[0:heads, at : at + width] = high
    ref[SLOT : SLOT + heads, at : at + width] = low


def layer_kernel(
    heads, width, length, depth, channels, shards,
    x_hbm, z_hbm, w_hbm, bc_hbm, bc_ref, dt_ref, a_ref, d_ref, cx_ref, cbc_ref, gain_ref, spread_ref, tri_ref,
    out_ref,
    x_own, z_own, w_own, halo_x, halo_bc, xpad, bcpad, fac, fac2, log_own, log_pair, masked, c_own, bt,
    conv, scaled, run, block_run, state, pair_state, base, chain_out, enter_in, entering, unit,
    sq_out, sq_in, sq_mid, sq_far, one_out, one_in, kept, two_out, two_in,
    local_sem, halo_send, halo_recv, pair_send, pair_recv, chain_send, chain_recv, swap_send, swap_recv,
    one_send, one_recv, two_send, two_recv,
):
    f32, bf16 = jnp.float32, jnp.bfloat16
    blocks = length // Q
    tile = out_ref.shape[1]
    pieces = width // LANES
    half = pieces // 2
    me = lax.axis_index("seq")
    parity = lax.rem(me, 2)
    pair = me // 2
    pairs = shards // 2
    own = lax.axis_index("head")
    near = own + 1 - 2 * lax.rem(own, 2)
    far = lax.rem(own + 2, 4)
    near_far = lax.rem(near + 2, 4)
    mate = me + 1 - 2 * parity

    barrier = pltpu.get_barrier_semaphore()

    def greet(target):
        pl.semaphore_signal(barrier, inc=1, device_id=target, device_id_type=pl.DeviceIdType.MESH)

    loads = [
        pltpu.make_async_copy(x_hbm, x_own, local_sem.at[0]),
        pltpu.make_async_copy(z_hbm, z_own, local_sem.at[1]),
        pltpu.make_async_copy(w_hbm, w_own, local_sem.at[2]),
    ]
    for load in loads:
        load.start()
    for jump in (1, 2):
        @pl.when(me >= jump)
        def _():
            greet({"seq": me - jump})

        @pl.when(me < shards - jump)
        def _():
            greet({"seq": me + jump})
    greet({"head": near})
    greet({"head": far})
    count = 2
    for jump in (1, 2):
        count = count + jnp.where(me >= jump, 1, 0) + jnp.where(me < shards - jump, 1, 0)
    pl.semaphore_wait(barrier, count)

    def remote(source, target, send, recv, device):
        return pltpu.make_async_remote_copy(
            src_ref=source, dst_ref=target, send_sem=send, recv_sem=recv,
            device_id=device, device_id_type=pl.DeviceIdType.MESH,
        )

    after = jnp.minimum(me + 1, shards - 1)
    halo = [
        remote(x_hbm.at[pl.ds(length - RIM, RIM)], halo_x, halo_send.at[0], halo_recv.at[0], {"seq": after}),
        remote(bc_hbm.at[pl.ds(length - RIM, RIM)], halo_bc, halo_send.at[1], halo_recv.at[1], {"seq": after}),
    ]

    @pl.when(me < shards - 1)
    def _():
        for copy in halo:
            copy.start()

    @pl.when(me == 0)
    def _():
        halo_x[...] = jnp.zeros_like(halo_x)
        halo_bc[...] = jnp.zeros_like(halo_bc)

    fac[...] = jnp.zeros_like(fac)
    fac2[...] = jnp.zeros_like(fac2)
    tri = tri_ref[...]
    before_log = jnp.zeros((heads, 1), f32)
    for block in range(blocks):
        dt = dt_ref[:, block * Q : (block + 1) * Q]
        step = jnp.maximum(dt, 0.0) + jnp.log1p(jnp.exp(-jnp.abs(dt)))
        rest = -jnp.exp(a_ref[...]) * step
        cum = jnp.zeros_like(rest)
        for _ in range(3):
            piece = rest.astype(bf16)
            cum = cum + jnp.dot(piece, tri, preferred_element_type=f32)
            rest = rest - piece.astype(f32)
        last = cum[:, Q - 1 : Q]
        mid = 0.5 * last
        here = fac.at[block]
        store_split(here, 0, jnp.exp(cum - mid), heads)
        store_split(here, Q, jnp.exp(mid - cum) * step, heads)
        lane = lax.broadcasted_iota(jnp.int32, (heads, LANES), 1)
        scal = jnp.where(lane == 0, last, jnp.where(lane == 1, mid, last - mid))
        store_split(here, 2 * Q, jnp.exp(scal), heads)
        store_split(fac2.at[block], 0, jnp.exp(before_log + cum), heads)
        before_log = before_log + last
    log_own[...] = jnp.broadcast_to(before_log, log_own.shape)

    def wide_row(logs, cols):
        value = jnp.exp(logs)
        high = value.astype(bf16)
        low = (value - high.astype(f32)).astype(bf16)
        both = dot_t(high, spread_ref[0:heads, cols]) + dot_t(low, spread_ref[0:heads, cols])
        return both[0:1]

    @pl.when(me > 0)
    def _():
        for copy in halo:
            copy.wait_recv()

    loads[0].wait()
    run[...] = jnp.zeros_like(run)

    @pl.loop(0, blocks)
    def _(block):
        start = pl.multiple_of(block * Q, Q)

        @pl.when(block == 0)
        def _():
            xpad[0:RIM, :] = halo_x[...].astype(f32)
            bcpad[0:RIM, :] = halo_bc[...].astype(f32)

        @pl.when(block > 0)
        def _():
            rim = pl.multiple_of(block * Q - RIM, RIM)
            xpad[0:RIM, :] = x_own[pl.ds(rim, RIM), :].astype(f32)
            bcpad[0:RIM, :] = bc_ref[pl.ds(rim, RIM), :].astype(f32)

        xpad[RIM : RIM + Q, :] = x_own[pl.ds(start, Q), :].astype(f32)
        bcpad[RIM : RIM + Q, :] = bc_ref[pl.ds(start, Q), :].astype(f32)
        bc = conv_rows(bcpad, cbc_ref[...], slice(None), Q)
        b_part = bc[:, :N].astype(bf16)
        c_part = bc[:, N:].astype(bf16)
        c_own[pl.ds(start, Q), :] = c_part
        bt[...] = bc[:, :N].T.astype(bf16)
        scores = lax.dot_general(c_part, b_part, (((1,), (1,)), ((), ())), preferred_element_type=f32)
        rows_at = lax.broadcasted_iota(jnp.int32, (Q, Q), 0)
        cols_at = lax.broadcasted_iota(jnp.int32, (Q, Q), 1)
        masked[block] = jnp.where(rows_at >= cols_at, scores, 0.0).astype(bf16)
        for col in range(0, width, CHUNK):
            cols = slice(col, col + CHUNK)
            wide = dot_t(fac[block, :, Q : 2 * Q + LANES], spread_ref[:, cols])
            xc = conv_rows(xpad, cx_ref[:, cols], cols, Q).astype(bf16)
            conv[pl.ds(start, Q), cols] = xc
            now = (xc.astype(f32) * wide[0:Q]).astype(bf16)
            scaled[pl.ds(start, Q), cols] = now
            held = run[:, cols]
            block_run[block, :, cols] = (held * wide[Q + 1 : Q + 2]).astype(bf16)
            added = jnp.dot(bt[...], now, preferred_element_type=f32)
            run[:, cols] = held * wide[Q : Q + 1] + wide[Q + 2 : Q + 3] * added

    for number in range(pieces):
        state[number] = run[:, number * LANES : (number + 1) * LANES].astype(bf16)

    first = parity * half
    other = half - first
    give = [
        remote(log_own, log_pair, pair_send.at[0], pair_recv.at[0], {"seq": mate}),
        remote(state.at[pl.ds(other, half)], pair_state.at[pl.ds(other, half)], pair_send.at[1], pair_recv.at[1], {"seq": mate}),
    ]
    give_rest = remote(state.at[pl.ds(first, half)], pair_state.at[pl.ds(first, half)], pair_send.at[2], pair_recv.at[2], {"seq": mate})
    take = [
        remote(log_own, log_pair, pair_send.at[0], pair_recv.at[0], {"seq": mate}),
        remote(state.at[pl.ds(first, half)], pair_state.at[pl.ds(first, half)], pair_send.at[1], pair_recv.at[1], {"seq": mate}),
    ]
    for copy in give:
        copy.start()

    @pl.when(parity == 0)
    def _():
        give_rest.start()

    def intra(block):
        start = pl.multiple_of(block * Q, Q)
        for col in range(0, width, CHUNK):
            cols = slice(col, col + CHUNK)
            wide = dot_t(fac[block, :, 0:Q], spread_ref[:, cols])
            y = jnp.dot(masked[block], scaled[pl.ds(start, Q), cols], preferred_element_type=f32)
            y = y + jnp.dot(c_own[pl.ds(start, Q), :], block_run[block, :, cols], preferred_element_type=f32)
            base[pl.ds(start, Q), cols] = wide * y + d_ref[:, cols] * conv[pl.ds(start, Q), cols].astype(f32)

    ahead = jnp.minimum(me + 2, shards - 1)

    def chain_copy(k):
        return remote(chain_out.at[k], enter_in.at[first + k], chain_send.at[k], chain_recv.at[k], {"seq": ahead})

    def swap_copy(k, at):
        return remote(enter_in.at[at + k], enter_in.at[at + k], swap_send.at[k], swap_recv.at[k], {"seq": mate})

    def exchange():
        for copy in take:
            copy.wait_recv()
        mine = log_own[...]
        theirs = log_pair[...]
        later = jnp.where(parity == 0, theirs, mine)

        @pl.when(pair == 0)
        def _():
            enter_in[...] = jnp.zeros_like(enter_in)

        for k in range(half):
            @pl.when(pair > 0)
            def _():
                chain_copy(k).wait_recv()
                swap_copy(k, first).start()

            @pl.when(pair < pairs - 1)
            def _():
                rows = jnp.where(parity == 0, wide_row(later, slice(k * LANES, (k + 1) * LANES)),
                                 wide_row(later, slice((half + k) * LANES, (half + k + 1) * LANES)))
                both = jnp.where(parity == 0, wide_row(mine + theirs, slice(k * LANES, (k + 1) * LANES)),
                                 wide_row(mine + theirs, slice((half + k) * LANES, (half + k + 1) * LANES)))
                mine_k = state[first + k].astype(f32)
                theirs_k = pair_state[first + k].astype(f32)
                early = jnp.where(parity == 0, mine_k, theirs_k)
                late = jnp.where(parity == 0, theirs_k, mine_k)
                total = both * enter_in[first + k].astype(f32) + rows * early + late
                chain_out[k] = total.astype(bf16)
                chain_copy(k).start()

    ready = jnp.minimum(pair, blocks)

    @pl.loop(0, blocks + 1)
    def _(turn):
        @pl.when(turn == ready)
        def _():
            exchange()

        @pl.when(turn < blocks)
        def _():
            intra(turn)

    @pl.when(pair > 0)
    def _():
        for k in range(half):
            swap_copy(k, other).wait_recv()

    @pl.when(parity == 1)
    def _():
        give_rest.wait_recv()
        for k in range(pieces):
            row = wide_row(log_pair[...], slice(k * LANES, (k + 1) * LANES))
            value = row * enter_in[k].astype(f32) + pair_state[k].astype(f32)
            entering[:, k * LANES : (k + 1) * LANES] = value.astype(bf16)

    @pl.when(parity == 0)
    def _():
        for k in range(pieces):
            entering[:, k * LANES : (k + 1) * LANES] = enter_in[k]

    loads[1].wait()
    loads[2].wait()

    def near_copies(block):
        return [
            remote(one_out.at[block], one_in.at[block], one_send.at[block, 0], one_recv.at[block, 0], {"head": near}),
            remote(sq_out.at[block], sq_in.at[block], one_send.at[block, 1], one_recv.at[block, 1], {"head": near}),
        ]

    def far_copies(block):
        return [
            remote(two_out.at[block], two_in.at[block], two_send.at[block, 0], two_recv.at[block, 0], {"head": far}),
            remote(sq_mid.at[block], sq_far.at[block], two_send.at[block, 1], two_recv.at[block, 1], {"head": far}),
        ]

    def product(index):
        at = pl.multiple_of(index * tile, LANES)
        return jnp.dot(unit[...], w_own[:, pl.ds(at, tile)], preferred_element_type=f32)

    @pl.loop(0, blocks)
    def _(block):
        start = pl.multiple_of(block * Q, Q)
        rows = pl.ds(start, Q)
        total = jnp.zeros((Q, LANES), f32)
        for col in range(0, width, CHUNK):
            cols = slice(col, col + CHUNK)
            wide = dot_t(fac2[block], spread_ref[:, cols])
            outer = jnp.dot(c_own[rows, :], entering[:, cols], preferred_element_type=f32)
            mixed = base[rows, cols] + wide * outer
            gated = mixed * silu(z_own[rows, cols].astype(f32))
            square = gated * gated
            for part in range(0, CHUNK, LANES):
                total = total + square[:, part : part + LANES]
            unit[:, cols] = (gated * gain_ref[:, cols]).astype(bf16)
        sq_out[block] = lax.dot_general(
            jnp.ones((8, LANES), f32), total, (((1,), (1,)), ((), ())),
            precision=lax.Precision.HIGHEST, preferred_element_type=f32,
        )
        one_out[block, 0] = product(near_far).astype(bf16)
        one_out[block, 1] = product(near).astype(bf16)
        for copy in near_copies(block):
            copy.start()
        two = product(far)
        kept[block] = product(own)
        for copy in near_copies(block):
            copy.wait_recv()
        two_out[block] = (two + one_in[block, 0].astype(f32)).astype(bf16)
        sq_mid[block] = sq_out[block] + sq_in[block]
        for copy in far_copies(block):
            copy.start()
        kept[block] = kept[block] + one_in[block, 1].astype(f32)

    @pl.loop(0, blocks)
    def _(block):
        start = pl.multiple_of(block * Q, Q)
        for copy in far_copies(block):
            copy.wait_recv()
        squares = sq_mid[block] + sq_far[block]
        column = lax.dot_general(
            squares, jnp.full((8, LANES), 0.125, f32), (((0,), (0,)), ((), ())),
            precision=lax.Precision.HIGHEST, preferred_element_type=f32,
        )
        scale = lax.rsqrt(column / channels + norm_floor)[:, 0:1]
        out_ref[pl.ds(start, Q), :] = ((kept[block] + two_in[block].astype(f32)) * scale).astype(bf16)

    @pl.loop(0, blocks)
    def _(block):
        for copy in near_copies(block) + far_copies(block):
            copy.wait_send()

    @pl.when(me < shards - 1)
    def _():
        for copy in halo:
            copy.wait_send()

    for copy in give:
        copy.wait_send()

    @pl.when(parity == 0)
    def _():
        give_rest.wait_send()

    for k in range(half):
        @pl.when(pair > 0)
        def _():
            swap_copy(k, first).wait_send()

        @pl.when(pair < pairs - 1)
        def _():
            chain_copy(k).wait_send()


def local(shards, channels, x_raw, bc_raw, z_gate, dt_raw, a_log, d_skip, conv_x, conv_bc, norm_gain, w_out):
    length, width = x_raw.shape
    heads = a_log.shape[0]
    blocks = length // Q
    depth = w_out.shape[1]
    tile = depth // lax.axis_size("head")
    pieces = width // LANES
    half = pieces // 2
    spread = np.zeros((2 * SLOT, width), np.float32)
    for head in range(heads):
        spread[head, head * P_SIZE : (head + 1) * P_SIZE] = 1.0
        spread[SLOT + head, head * P_SIZE : (head + 1) * P_SIZE] = 1.0
    spread = jnp.asarray(spread, jnp.bfloat16)
    tri = jnp.asarray(np.triu(np.ones((Q, Q), np.float32)), jnp.bfloat16)
    d_wide = jnp.repeat(d_skip, P_SIZE)[None]
    f32, bf16 = jnp.float32, jnp.bfloat16
    anywhere = pl.BlockSpec(memory_space=pl.ANY)
    inside = pl.BlockSpec(memory_space=pltpu.VMEM)
    vmem = pltpu.VMEM
    dma = pltpu.SemaphoreType.DMA
    return pl.pallas_call(
        functools.partial(layer_kernel, heads, width, length, depth, channels, shards),
        in_specs=[anywhere] * 4 + [inside] * 9,
        out_specs=inside,
        out_shape=jax.ShapeDtypeStruct((length, tile), bf16),
        scratch_shapes=[
            vmem((length, width), bf16),
            vmem((length, width), bf16),
            vmem((width, depth), bf16),
            vmem((RIM, width), bf16),
            vmem((RIM, 2 * N), bf16),
            vmem((RIM + Q, width), f32),
            vmem((RIM + Q, 2 * N), f32),
            vmem((blocks, 2 * SLOT, 2 * Q + LANES), bf16),
            vmem((blocks, 2 * SLOT, Q), bf16),
            vmem((heads, LANES), f32),
            vmem((heads, LANES), f32),
            vmem((blocks, Q, Q), bf16),
            vmem((length, N), bf16),
            vmem((N, Q), bf16),
            vmem((length, width), bf16),
            vmem((length, width), bf16),
            vmem((N, width), f32),
            vmem((blocks, N, width), bf16),
            vmem((pieces, N, LANES), bf16),
            vmem((pieces, N, LANES), bf16),
            vmem((length, width), f32),
            vmem((half, N, LANES), bf16),
            vmem((pieces, N, LANES), bf16),
            vmem((N, width), bf16),
            vmem((Q, width), bf16),
            vmem((blocks, 8, Q), f32),
            vmem((blocks, 8, Q), f32),
            vmem((blocks, 8, Q), f32),
            vmem((blocks, 8, Q), f32),
            vmem((blocks, 2, Q, tile), bf16),
            vmem((blocks, 2, Q, tile), bf16),
            vmem((blocks, Q, tile), f32),
            vmem((blocks, Q, tile), bf16),
            vmem((blocks, Q, tile), bf16),
            dma((3,)), dma((2,)), dma((2,)), dma((3,)), dma((3,)),
            dma((half,)), dma((half,)), dma((half,)), dma((half,)),
            dma((blocks, 2)), dma((blocks, 2)), dma((blocks, 2)), dma((blocks, 2)),
        ],
        compiler_params=pltpu.CompilerParams(
            collective_id=0, has_side_effects=True, vmem_limit_bytes=63 << 20
        ),
    )(x_raw, z_gate, w_out, bc_raw, bc_raw, dt_raw, a_log[:, None], d_wide, conv_x, conv_bc, norm_gain[None], spread, tri)


def solution(mesh):
    in_specs = (
        P("seq", "head"),
        P("seq", None),
        P("seq", "head"),
        P("head", "seq"),
        P("head"),
        P("head"),
        P(None, "head"),
        P(),
        P("head"),
        P("head", None),
    )

    def whole(x_raw, *rest):
        body = functools.partial(local, mesh.shape["seq"], x_raw.shape[1])
        return jax.shard_map(
            body, mesh=mesh, in_specs=in_specs, out_specs=P("seq", "head"), check_vma=False
        )(x_raw, *rest)

    return whole
```

```python
import functools

import jax
import jax.numpy as jnp
import numpy as np
from jax import lax
from jax.experimental import pallas as pl
from jax.experimental.pallas import tpu as pltpu
from jax.sharding import PartitionSpec as P

P_SIZE = 64
N = 128
Q = 256
CONV = 4
RIM = 16
LANES = 128
CHUNK = 256
SLOT = 32

norm_floor = 0.5


def silu(v):
    return v / (1.0 + jnp.exp(-v))


def dot_t(a, b):
    return lax.dot_general(a, b, (((0,), (0,)), ((), ())), preferred_element_type=jnp.float32)


def conv_rows(padded_ref, taps, at):
    first = RIM - CONV + 1 + at
    total = padded_ref[first : first + Q, :] * taps[0:1]
    for number in range(1, CONV):
        total = total + padded_ref[first + number : first + number + Q, :] * taps[number : number + 1]
    return silu(total)


def store_split(ref, at, value, heads):
    high = value.astype(jnp.bfloat16)
    low = (value - high.astype(jnp.float32)).astype(jnp.bfloat16)
    width = value.shape[1]
    ref[0:heads, at : at + width] = high
    ref[SLOT : SLOT + heads, at : at + width] = low


def layer_kernel(
    heads, width, length, depth, channels, shards,
    x_hbm, z_hbm, w_hbm, bc_hbm, bc_ref, dt_ref, a_ref, d_ref, cx_ref, cbc_ref, gain_ref, spread_ref, tri_ref,
    out_ref,
    x_own, z_own, w_own, halo_x, halo_bc, xpad, bcpad, fac, fac2, log_own, log_pair, masked, c_own, bt,
    conv, scaled, block_run, state, pair_state, row_pair, row_first, pair_total, base, chain_out, enter_in, entering, unit,
    sq_out, sq_in, sq_mid, sq_far, one_out, one_in, kept, two_out, two_in,
    local_sem, halo_send, halo_recv, pair_send, pair_recv, chain_send, chain_recv, swap_send, swap_recv,
    one_send, one_recv, two_send, two_recv, log_sem,
):
    f32, bf16 = jnp.float32, jnp.bfloat16
    blocks = length // Q
    tile = out_ref.shape[1]
    pieces = width // LANES
    half = pieces // 2
    me = lax.axis_index("seq")
    parity = lax.rem(me, 2)
    pair = me // 2
    pairs = shards // 2
    own = lax.axis_index("head")
    near = own + 1 - 2 * lax.rem(own, 2)
    far = lax.rem(own + 2, 4)
    near_far = lax.rem(near + 2, 4)
    mate = me + 1 - 2 * parity

    barrier = pltpu.get_barrier_semaphore()

    def greet(target):
        pl.semaphore_signal(barrier, inc=1, device_id=target, device_id_type=pl.DeviceIdType.MESH)

    loads = [
        pltpu.make_async_copy(x_hbm, x_own, local_sem.at[0]),
        pltpu.make_async_copy(z_hbm, z_own, local_sem.at[1]),
        pltpu.make_async_copy(w_hbm, w_own, local_sem.at[2]),
    ]
    for load in loads:
        load.start()
    for jump in (1, 2):
        @pl.when(me >= jump)
        def _():
            greet({"seq": me - jump})

        @pl.when(me < shards - jump)
        def _():
            greet({"seq": me + jump})
    greet({"head": near})
    greet({"head": far})
    count = 2
    for jump in (1, 2):
        count = count + jnp.where(me >= jump, 1, 0) + jnp.where(me < shards - jump, 1, 0)
    pl.semaphore_wait(barrier, count)

    def remote(source, target, send, recv, device):
        return pltpu.make_async_remote_copy(
            src_ref=source, dst_ref=target, send_sem=send, recv_sem=recv,
            device_id=device, device_id_type=pl.DeviceIdType.MESH,
        )

    after = jnp.minimum(me + 1, shards - 1)
    halo = [
        remote(x_hbm.at[pl.ds(length - RIM, RIM)], halo_x, halo_send.at[0], halo_recv.at[0], {"seq": after}),
        remote(bc_hbm.at[pl.ds(length - RIM, RIM)], halo_bc, halo_send.at[1], halo_recv.at[1], {"seq": after}),
    ]

    @pl.when(me < shards - 1)
    def _():
        for copy in halo:
            copy.start()

    @pl.when(me == 0)
    def _():
        halo_x[...] = jnp.zeros_like(halo_x)
        halo_bc[...] = jnp.zeros_like(halo_bc)

    head_at = lax.broadcasted_iota(jnp.int32, (heads, 1), 0)
    a_col = jnp.zeros((heads, 1), f32)
    d_col = jnp.zeros((heads, 1), f32)
    for head in range(heads):
        a_col = jnp.where(head_at == head, a_ref[head], a_col)
        d_col = jnp.where(head_at == head, d_ref[head], d_col)
    minus_a = -jnp.exp(a_col)
    fac[...] = jnp.zeros_like(fac)
    fac2[...] = jnp.zeros_like(fac2)
    tri = tri_ref[...]
    before_log = jnp.zeros((heads, 1), f32)
    for block in range(blocks):
        dt = dt_ref[:, block * Q : (block + 1) * Q]
        step = jnp.maximum(dt, 0.0) + jnp.log1p(jnp.exp(-jnp.abs(dt)))
        rest = minus_a * step
        cum = jnp.zeros_like(rest)
        for _ in range(3):
            piece = rest.astype(bf16)
            cum = cum + jnp.dot(piece, tri, preferred_element_type=f32)
            rest = rest - piece.astype(f32)
        last = cum[:, Q - 1 : Q]
        mid = 0.5 * last
        here = fac.at[block]
        store_split(here, 0, jnp.exp(cum - mid), heads)
        store_split(here, Q, jnp.exp(mid - cum) * step, heads)
        lane = lax.broadcasted_iota(jnp.int32, (heads, LANES), 1)
        scal = jnp.where(lane == 0, last, jnp.where(lane == 1, mid, last - mid))
        store_split(here, 2 * Q, jnp.exp(scal), heads)
        store_split(fac2.at[block], 0, jnp.exp(before_log + cum), heads)
        before_log = before_log + last
    log_own[...] = jnp.broadcast_to(before_log, log_own.shape)
    give_log = remote(log_own, log_pair, log_sem.at[0], log_sem.at[1], {"seq": mate})
    give_log.start()

    def wide_row(value, cols):
        high = value.astype(bf16)
        low = (value - high.astype(f32)).astype(bf16)
        both = dot_t(high, spread_ref[0:heads, cols]) + dot_t(low, spread_ref[0:heads, cols])
        return both[0:1]

    @pl.when(me > 0)
    def _():
        for copy in halo:
            copy.wait_recv()

    bcpad[0:RIM, :] = halo_bc[...].astype(f32)
    bcpad[RIM : RIM + length, :] = bc_ref[...].astype(f32)
    for block in range(blocks):
        rows = slice(block * Q, (block + 1) * Q)
        bc = conv_rows(bcpad, cbc_ref[...], block * Q)
        c_own[rows, :] = bc[:, N:].astype(bf16)
        bt[:, rows] = bc[:, :N].T.astype(bf16)
    d_wide = wide_row(jnp.broadcast_to(d_col, (heads, LANES)), slice(0, width))
    loads[0].wait()

    first = parity * half
    other = half - first

    def state_copy(index):
        return remote(state.at[index], pair_state.at[index], pair_send.at[index], pair_recv.at[index], {"seq": mate})

    @pl.loop(0, pieces)
    def _(number):
        index = lax.rem(other + number, pieces)
        cols = pl.ds(pl.multiple_of(index * LANES, LANES), LANES)
        xpad[0:RIM, :] = halo_x[:, cols].astype(f32)
        xpad[RIM : RIM + length, :] = x_own[:, cols].astype(f32)
        taps = cx_ref[:, cols]
        held = jnp.zeros((N, LANES), f32)
        for block in range(blocks):
            rows = slice(block * Q, (block + 1) * Q)
            wide = dot_t(fac[block, :, Q : 2 * Q + LANES], spread_ref[:, cols])
            xc = conv_rows(xpad, taps, block * Q).astype(bf16)
            conv[rows, cols] = xc
            now = (xc.astype(f32) * wide[0:Q]).astype(bf16)
            scaled[rows, cols] = now
            block_run[block, index] = (held * wide[Q + 1 : Q + 2]).astype(bf16)
            added = jnp.dot(bt[:, rows], now, preferred_element_type=f32)
            held = held * wide[Q : Q + 1] + wide[Q + 2 : Q + 3] * added
        state[index] = held.astype(bf16)

        @pl.when((number < half) | (parity == 0))
        def _():
            state_copy(index).start()

    def intra(block):
        start = pl.multiple_of(block * Q, Q)
        rows = pl.ds(start, Q)
        c_part = c_own[rows, :]
        scores = jnp.dot(c_part, bt[:, rows], preferred_element_type=f32)
        rows_at = lax.broadcasted_iota(jnp.int32, (Q, Q), 0)
        cols_at = lax.broadcasted_iota(jnp.int32, (Q, Q), 1)
        masked[...] = jnp.where(rows_at >= cols_at, scores, 0.0).astype(bf16)
        for col in range(0, width, CHUNK):
            cols = slice(col, col + CHUNK)
            wide = dot_t(fac[block, :, 0:Q], spread_ref[:, cols])
            y = jnp.dot(masked[...], scaled[rows, cols], preferred_element_type=f32)
            at = col // LANES
            held = jnp.concatenate([block_run[block, at], block_run[block, at + 1]], axis=1)
            y = y + jnp.dot(c_part, held, preferred_element_type=f32)
            base[rows, cols] = wide * y + d_wide[:, cols] * conv[rows, cols].astype(f32)

    ahead = jnp.minimum(me + 2, shards - 1)

    def chain_copy(k):
        return remote(chain_out.at[k], enter_in.at[first + k], chain_send.at[k], chain_recv.at[k], {"seq": ahead})

    def swap_copy(k, at):
        return remote(enter_in.at[at + k], enter_in.at[at + k], swap_send.at[k], swap_recv.at[k], {"seq": mate})

    give_log.wait_recv()
    mine = log_own[...]
    theirs = log_pair[...]
    row_of_pair = jnp.exp(mine + theirs)
    row_of_late = jnp.exp(jnp.where(parity == 0, theirs, mine))
    row_of_early = jnp.exp(theirs)

    @pl.loop(0, half)
    def _(k):
        cols = pl.ds(pl.multiple_of((first + k) * LANES, LANES), LANES)
        state_copy(first + k).wait_recv()
        row_pair[k] = jnp.broadcast_to(wide_row(row_of_pair, cols), (8, LANES))
        mine_k = state[first + k].astype(f32)
        theirs_k = pair_state[first + k].astype(f32)
        early = jnp.where(parity == 0, mine_k, theirs_k)
        late = jnp.where(parity == 0, theirs_k, mine_k)
        pair_total[k] = wide_row(row_of_late, cols) * early + late

    @pl.when(pair == 0)
    def _():
        enter_in[...] = jnp.zeros_like(enter_in)

    def exchange():
        @pl.loop(0, half)
        def _(k):
            @pl.when(pair > 0)
            def _():
                chain_copy(k).wait_recv()

            @pl.when(pair < pairs - 1)
            def _():
                total = row_pair[k, 0:1] * enter_in[first + k].astype(f32) + pair_total[k]
                chain_out[k] = total.astype(bf16)
                chain_copy(k).start()

            @pl.when(pair > 0)
            def _():
                swap_copy(k, first).start()

        @pl.when(parity == 1)
        def _():
            for k in range(pieces):
                row = wide_row(row_of_early, slice(k * LANES, (k + 1) * LANES))
                row_first[k] = jnp.broadcast_to(row, (8, LANES))

    ready = jnp.minimum(pair, blocks)

    @pl.loop(0, blocks + 1)
    def _(turn):
        @pl.when(turn == ready)
        def _():
            exchange()

        @pl.when(turn < blocks)
        def _():
            intra(turn)

    @pl.when(pair > 0)
    def _():
        for k in range(half):
            swap_copy(k, other).wait_recv()

    @pl.when(parity == 1)
    def _():
        for k in range(half):
            state_copy(other + k).wait_recv()
        for k in range(pieces):
            value = row_first[k, 0:1] * enter_in[k].astype(f32) + pair_state[k].astype(f32)
            entering[:, k * LANES : (k + 1) * LANES] = value.astype(bf16)

    @pl.when(parity == 0)
    def _():
        for k in range(pieces):
            entering[:, k * LANES : (k + 1) * LANES] = enter_in[k]

    gain = gain_ref[...].reshape(1, width)
    loads[1].wait()
    loads[2].wait()

    def near_copies(block):
        return [
            remote(one_out.at[block, 0], one_in.at[block, 0], one_send.at[block, 0], one_recv.at[block, 0], {"head": near}),
            remote(sq_out.at[block], sq_in.at[block], one_send.at[block, 1], one_recv.at[block, 1], {"head": near}),
            remote(one_out.at[block, 1], one_in.at[block, 1], one_send.at[block, 2], one_recv.at[block, 2], {"head": near}),
        ]

    def far_copies(block):
        return [
            remote(two_out.at[block], two_in.at[block], two_send.at[block, 0], two_recv.at[block, 0], {"head": far}),
            remote(sq_mid.at[block], sq_far.at[block], two_send.at[block, 1], two_recv.at[block, 1], {"head": far}),
        ]

    def product(index):
        at = pl.multiple_of(index * tile, LANES)
        return jnp.dot(unit[...], w_own[:, pl.ds(at, tile)], preferred_element_type=f32)

    @pl.loop(0, blocks)
    def _(block):
        start = pl.multiple_of(block * Q, Q)
        rows = pl.ds(start, Q)
        total = jnp.zeros((Q, LANES), f32)
        for col in range(0, width, CHUNK):
            cols = slice(col, col + CHUNK)
            wide = dot_t(fac2[block], spread_ref[:, cols])
            outer = jnp.dot(c_own[rows, :], entering[:, cols], preferred_element_type=f32)
            mixed = base[rows, cols] + wide * outer
            gated = mixed * silu(z_own[rows, cols].astype(f32))
            square = gated * gated
            for part in range(0, CHUNK, LANES):
                total = total + square[:, part : part + LANES]
            unit[:, cols] = (gated * gain[:, cols]).astype(bf16)
        sq_out[block] = lax.dot_general(
            jnp.ones((8, LANES), f32), total, (((1,), (1,)), ((), ())),
            precision=lax.Precision.HIGHEST, preferred_element_type=f32,
        )
        copies = near_copies(block)
        one_out[block, 0] = product(near_far).astype(bf16)
        copies[0].start()
        copies[1].start()
        two = product(far)
        copies[0].wait_recv()
        two_out[block] = (two + one_in[block, 0].astype(f32)).astype(bf16)
        copies[1].wait_recv()
        sq_mid[block] = sq_out[block] + sq_in[block]
        for copy in far_copies(block):
            copy.start()
        one_out[block, 1] = product(near).astype(bf16)
        copies[2].start()
        kept[block] = product(own)

    @pl.loop(0, blocks)
    def _(block):
        start = pl.multiple_of(block * Q, Q)
        near_copies(block)[2].wait_recv()
        for copy in far_copies(block):
            copy.wait_recv()
        squares = sq_mid[block] + sq_far[block]
        column = lax.dot_general(
            squares, jnp.full((8, LANES), 0.125, f32), (((0,), (0,)), ((), ())),
            precision=lax.Precision.HIGHEST, preferred_element_type=f32,
        )
        scale = lax.rsqrt(column / channels + norm_floor)[:, 0:1]
        out_ref[pl.ds(start, Q), :] = ((kept[block] + one_in[block, 1].astype(f32) + two_in[block].astype(f32)) * scale).astype(bf16)

    @pl.loop(0, blocks)
    def _(block):
        for copy in near_copies(block) + far_copies(block):
            copy.wait_send()

    @pl.when(me < shards - 1)
    def _():
        for copy in halo:
            copy.wait_send()

    give_log.wait_send()
    for k in range(half):
        state_copy(other + k).wait_send()

        @pl.when(parity == 0)
        def _():
            state_copy(first + k).wait_send()

    for k in range(half):
        @pl.when(pair > 0)
        def _():
            swap_copy(k, first).wait_send()

        @pl.when(pair < pairs - 1)
        def _():
            chain_copy(k).wait_send()


def local(shards, channels, x_raw, bc_raw, z_gate, dt_raw, a_log, d_skip, conv_x, conv_bc, norm_gain, w_out):
    length, width = x_raw.shape
    heads = a_log.shape[0]
    blocks = length // Q
    depth = w_out.shape[1]
    tile = depth // lax.axis_size("head")
    pieces = width // LANES
    half = pieces // 2
    spread = np.zeros((2 * SLOT, width), np.float32)
    for head in range(heads):
        spread[head, head * P_SIZE : (head + 1) * P_SIZE] = 1.0
        spread[SLOT + head, head * P_SIZE : (head + 1) * P_SIZE] = 1.0
    spread = jnp.asarray(spread, jnp.bfloat16)
    tri = jnp.asarray(np.triu(np.ones((Q, Q), np.float32)), jnp.bfloat16)
    f32, bf16 = jnp.float32, jnp.bfloat16
    anywhere = pl.BlockSpec(memory_space=pl.ANY)
    inside = pl.BlockSpec(memory_space=pltpu.VMEM)
    scalars = pl.BlockSpec(memory_space=pltpu.SMEM)
    vmem = pltpu.VMEM
    dma = pltpu.SemaphoreType.DMA
    return pl.pallas_call(
        functools.partial(layer_kernel, heads, width, length, depth, channels, shards),
        in_specs=[anywhere] * 4 + [inside] * 2 + [scalars] * 2 + [inside] * 5,
        out_specs=inside,
        out_shape=jax.ShapeDtypeStruct((length, tile), bf16),
        scratch_shapes=[
            vmem((length, width), bf16),
            vmem((length, width), bf16),
            vmem((width, depth), bf16),
            vmem((RIM, width), bf16),
            vmem((RIM, 2 * N), bf16),
            vmem((RIM + length, LANES), f32),
            vmem((RIM + length, 2 * N), f32),
            vmem((blocks, 2 * SLOT, 2 * Q + LANES), bf16),
            vmem((blocks, 2 * SLOT, Q), bf16),
            vmem((heads, LANES), f32),
            vmem((heads, LANES), f32),
            vmem((Q, Q), bf16),
            vmem((length, N), bf16),
            vmem((N, length), bf16),
            vmem((length, width), bf16),
            vmem((length, width), bf16),
            vmem((blocks, pieces, N, LANES), bf16),
            vmem((pieces, N, LANES), bf16),
            vmem((pieces, N, LANES), bf16),
            vmem((half, 8, LANES), f32),
            vmem((pieces, 8, LANES), f32),
            vmem((half, N, LANES), f32),
            vmem((length, width), f32),
            vmem((half, N, LANES), bf16),
            vmem((pieces, N, LANES), bf16),
            vmem((N, width), bf16),
            vmem((Q, width), bf16),
            vmem((blocks, 8, Q), f32),
            vmem((blocks, 8, Q), f32),
            vmem((blocks, 8, Q), f32),
            vmem((blocks, 8, Q), f32),
            vmem((blocks, 2, Q, tile), bf16),
            vmem((blocks, 2, Q, tile), bf16),
            vmem((blocks, Q, tile), f32),
            vmem((blocks, Q, tile), bf16),
            vmem((blocks, Q, tile), bf16),
            dma((3,)), dma((2,)), dma((2,)), dma((pieces,)), dma((pieces,)),
            dma((half,)), dma((half,)), dma((half,)), dma((half,)),
            dma((blocks, 3)), dma((blocks, 3)), dma((blocks, 2)), dma((blocks, 2)), dma((2,)),
        ],
        compiler_params=pltpu.CompilerParams(
            collective_id=0, has_side_effects=True, vmem_limit_bytes=63 << 20
        ),
    )(x_raw, z_gate, w_out, bc_raw, bc_raw, dt_raw, a_log, d_skip, conv_x, conv_bc, norm_gain, spread, tri)


def solution(mesh):
    in_specs = (
        P("seq", "head"),
        P("seq", None),
        P("seq", "head"),
        P("head", "seq"),
        P("head"),
        P("head"),
        P(None, "head"),
        P(),
        P("head"),
        P("head", None),
    )

    def whole(x_raw, *rest):
        body = functools.partial(local, mesh.shape["seq"], x_raw.shape[1])
        return jax.shard_map(
            body, mesh=mesh, in_specs=in_specs, out_specs=P("seq", "head"), check_vma=False
        )(x_raw, *rest)

    return whole
```

```python
import functools

import jax
import jax.numpy as jnp
import numpy as np
from jax import lax
from jax.experimental import pallas as pl
from jax.experimental.pallas import tpu as pltpu
from jax.sharding import PartitionSpec as P

P_SIZE = 64
N = 128
Q = 256
CONV = 4
RIM = 16
LANES = 128
CHUNK = 256
SLOT = 32

norm_floor = 0.5


def silu(v):
    part = 0.5 * v
    return part + part * jnp.tanh(part)


def dot_t(a, b):
    return lax.dot_general(a, b, (((0,), (0,)), ((), ())), preferred_element_type=jnp.float32)


def conv_rows(padded_ref, taps, at):
    first = RIM - CONV + 1 + at
    total = padded_ref[first : first + Q, :] * taps[0:1]
    for number in range(1, CONV):
        total = total + padded_ref[first + number : first + number + Q, :] * taps[number : number + 1]
    return silu(total)


def store_split(ref, at, value, heads):
    high = value.astype(jnp.bfloat16)
    low = (value - high.astype(jnp.float32)).astype(jnp.bfloat16)
    width = value.shape[1]
    ref[0:heads, at : at + width] = high
    ref[SLOT : SLOT + heads, at : at + width] = low


def layer_kernel(
    heads, width, length, depth, channels, shards,
    x_hbm, z_hbm, w_hbm, bc_hbm, bc_ref, dt_ref, a_ref, d_ref, cx_ref, cbc_ref, gain_ref, spread_ref, tri_ref,
    out_ref,
    x_own, z_own, w_own, halo_x, halo_bc, xpad, bcpad, fac, fac2, log_own, log_pair, masked, c_own, bt,
    conv, scaled, block_run, state, pair_state, row_pair, row_first, pair_total, base, chain_out, enter_in, entering, unit,
    sq_out, sq_in, sq_mid, sq_far, one_out, one_in, kept, two_out, two_in,
    local_sem, halo_send, halo_recv, pair_send, pair_recv, chain_send, chain_recv, swap_send, swap_recv,
    one_send, one_recv, two_send, two_recv, log_sem,
):
    f32, bf16 = jnp.float32, jnp.bfloat16
    blocks = length // Q
    tile = out_ref.shape[1]
    pieces = width // LANES
    half = pieces // 2
    me = lax.axis_index("seq")
    parity = lax.rem(me, 2)
    pair = me // 2
    pairs = shards // 2
    own = lax.axis_index("head")
    near = own + 1 - 2 * lax.rem(own, 2)
    far = lax.rem(own + 2, 4)
    near_far = lax.rem(near + 2, 4)
    mate = me + 1 - 2 * parity

    barrier = pltpu.get_barrier_semaphore()

    def greet(target):
        pl.semaphore_signal(barrier, inc=1, device_id=target, device_id_type=pl.DeviceIdType.MESH)

    loads = [
        pltpu.make_async_copy(x_hbm, x_own, local_sem.at[0]),
        pltpu.make_async_copy(z_hbm, z_own, local_sem.at[1]),
        pltpu.make_async_copy(w_hbm, w_own, local_sem.at[2]),
    ]
    for load in loads:
        load.start()
    for jump in (1, 2):
        @pl.when(me >= jump)
        def _():
            greet({"seq": me - jump})

        @pl.when(me < shards - jump)
        def _():
            greet({"seq": me + jump})
    greet({"head": near})
    greet({"head": far})
    count = 2
    for jump in (1, 2):
        count = count + jnp.where(me >= jump, 1, 0) + jnp.where(me < shards - jump, 1, 0)
    pl.semaphore_wait(barrier, count)

    def remote(source, target, send, recv, device):
        return pltpu.make_async_remote_copy(
            src_ref=source, dst_ref=target, send_sem=send, recv_sem=recv,
            device_id=device, device_id_type=pl.DeviceIdType.MESH,
        )

    after = jnp.minimum(me + 1, shards - 1)
    halo = [
        remote(x_hbm.at[pl.ds(length - RIM, RIM)], halo_x, halo_send.at[0], halo_recv.at[0], {"seq": after}),
        remote(bc_hbm.at[pl.ds(length - RIM, RIM)], halo_bc, halo_send.at[1], halo_recv.at[1], {"seq": after}),
    ]

    @pl.when(me < shards - 1)
    def _():
        for copy in halo:
            copy.start()

    @pl.when(me == 0)
    def _():
        halo_x[...] = jnp.zeros_like(halo_x)
        halo_bc[...] = jnp.zeros_like(halo_bc)

    head_at = lax.broadcasted_iota(jnp.int32, (heads, 1), 0)
    a_col = jnp.zeros((heads, 1), f32)
    d_col = jnp.zeros((heads, 1), f32)
    for head in range(heads):
        a_col = jnp.where(head_at == head, a_ref[head], a_col)
        d_col = jnp.where(head_at == head, d_ref[head], d_col)
    minus_a = -jnp.exp(a_col)
    fac[...] = jnp.zeros_like(fac)
    fac2[...] = jnp.zeros_like(fac2)
    tri = tri_ref[...]
    before_log = jnp.zeros((heads, 1), f32)
    for block in range(blocks):
        dt = dt_ref[:, block * Q : (block + 1) * Q]
        step = jnp.maximum(dt, 0.0) + jnp.log1p(jnp.exp(-jnp.abs(dt)))
        rest = minus_a * step
        cum = jnp.zeros_like(rest)
        for _ in range(3):
            piece = rest.astype(bf16)
            cum = cum + jnp.dot(piece, tri, preferred_element_type=f32)
            rest = rest - piece.astype(f32)
        last = cum[:, Q - 1 : Q]
        mid = 0.5 * last
        here = fac.at[block]
        store_split(here, 0, jnp.exp(cum - mid), heads)
        store_split(here, Q, jnp.exp(mid - cum) * step, heads)
        lane = lax.broadcasted_iota(jnp.int32, (heads, LANES), 1)
        scal = jnp.where(lane == 0, last, jnp.where(lane == 1, mid, last - mid))
        store_split(here, 2 * Q, jnp.exp(scal), heads)
        store_split(fac2.at[block], 0, jnp.exp(before_log + cum), heads)
        before_log = before_log + last
    log_own[...] = jnp.broadcast_to(before_log, log_own.shape)
    give_log = remote(log_own, log_pair, log_sem.at[0], log_sem.at[1], {"seq": mate})
    give_log.start()

    def wide_row(value, cols):
        high = value.astype(bf16)
        low = (value - high.astype(f32)).astype(bf16)
        both = dot_t(high, spread_ref[0:heads, cols]) + dot_t(low, spread_ref[0:heads, cols])
        return both[0:1]

    @pl.when(me > 0)
    def _():
        for copy in halo:
            copy.wait_recv()

    bcpad[0:RIM, :] = halo_bc[...].astype(f32)
    bcpad[RIM : RIM + length, :] = bc_ref[...].astype(f32)
    for block in range(blocks):
        rows = slice(block * Q, (block + 1) * Q)
        bc = conv_rows(bcpad, cbc_ref[...], block * Q)
        c_own[rows, :] = bc[:, N:].astype(bf16)
        bt[:, rows] = bc[:, :N].T.astype(bf16)
    d_wide = wide_row(jnp.broadcast_to(d_col, (heads, LANES)), slice(0, width))
    loads[0].wait()

    first = parity * half
    other = half - first

    def state_copy(index):
        return remote(state.at[index], pair_state.at[index], pair_send.at[index], pair_recv.at[index], {"seq": mate})

    @pl.loop(0, pieces)
    def _(number):
        index = lax.rem(other + number, pieces)
        cols = pl.ds(pl.multiple_of(index * LANES, LANES), LANES)
        xpad[0:RIM, :] = halo_x[:, cols].astype(f32)
        xpad[RIM : RIM + length, :] = x_own[:, cols].astype(f32)
        taps = cx_ref[:, cols]
        held = jnp.zeros((N, LANES), f32)
        for block in range(blocks):
            rows = slice(block * Q, (block + 1) * Q)
            wide = dot_t(fac[block, :, Q : 2 * Q + LANES], spread_ref[:, cols])
            xc = conv_rows(xpad, taps, block * Q).astype(bf16)
            conv[rows, cols] = xc
            now = (xc.astype(f32) * wide[0:Q]).astype(bf16)
            scaled[rows, cols] = now
            block_run[block, index] = (held * wide[Q + 1 : Q + 2]).astype(bf16)
            added = jnp.dot(bt[:, rows], now, preferred_element_type=f32)
            held = held * wide[Q : Q + 1] + wide[Q + 2 : Q + 3] * added
        state[index] = held.astype(bf16)

        @pl.when((number < half) | (parity == 0))
        def _():
            state_copy(index).start()

    def intra(block):
        start = pl.multiple_of(block * Q, Q)
        rows = pl.ds(start, Q)
        c_part = c_own[rows, :]
        scores = jnp.dot(c_part, bt[:, rows], preferred_element_type=f32)
        rows_at = lax.broadcasted_iota(jnp.int32, (Q, Q), 0)
        cols_at = lax.broadcasted_iota(jnp.int32, (Q, Q), 1)
        masked[...] = jnp.where(rows_at >= cols_at, scores, 0.0).astype(bf16)
        for col in range(0, width, CHUNK):
            cols = slice(col, col + CHUNK)
            wide = dot_t(fac[block, :, 0:Q], spread_ref[:, cols])
            y = jnp.dot(masked[...], scaled[rows, cols], preferred_element_type=f32)
            at = col // LANES
            held = jnp.concatenate([block_run[block, at], block_run[block, at + 1]], axis=1)
            y = y + jnp.dot(c_part, held, preferred_element_type=f32)
            base[rows, cols] = wide * y + d_wide[:, cols] * conv[rows, cols].astype(f32)

    ahead = jnp.minimum(me + 2, shards - 1)

    def chain_copy(k):
        return remote(chain_out.at[k], enter_in.at[first + k], chain_send.at[k], chain_recv.at[k], {"seq": ahead})

    def swap_copy(k, at):
        return remote(enter_in.at[at + k], enter_in.at[at + k], swap_send.at[k], swap_recv.at[k], {"seq": mate})

    give_log.wait_recv()
    mine = log_own[...]
    theirs = log_pair[...]
    row_of_pair = jnp.exp(mine + theirs)
    row_of_late = jnp.exp(jnp.where(parity == 0, theirs, mine))
    row_of_early = jnp.exp(theirs)

    @pl.loop(0, half)
    def _(k):
        cols = pl.ds(pl.multiple_of((first + k) * LANES, LANES), LANES)
        state_copy(first + k).wait_recv()
        row_pair[k] = jnp.broadcast_to(wide_row(row_of_pair, cols), (8, LANES))
        mine_k = state[first + k].astype(f32)
        theirs_k = pair_state[first + k].astype(f32)
        early = jnp.where(parity == 0, mine_k, theirs_k)
        late = jnp.where(parity == 0, theirs_k, mine_k)
        pair_total[k] = wide_row(row_of_late, cols) * early + late

    @pl.when(pair == 0)
    def _():
        enter_in[...] = jnp.zeros_like(enter_in)

    def early_rows():
        for col in range(0, width, CHUNK):
            row = wide_row(row_of_early, slice(col, col + CHUNK))
            for at in range(0, CHUNK, LANES):
                row_first[(col + at) // LANES] = jnp.broadcast_to(row[:, at : at + LANES], (8, LANES))

    def exchange():
        @pl.when((parity == 1) & (pair == pairs - 1))
        def _():
            early_rows()

        @pl.loop(0, half)
        def _(k):
            @pl.when(pair > 0)
            def _():
                chain_copy(k).wait_recv()

            @pl.when(pair < pairs - 1)
            def _():
                total = row_pair[k, 0:1] * enter_in[first + k].astype(f32) + pair_total[k]
                chain_out[k] = total.astype(bf16)
                chain_copy(k).start()

            @pl.when(pair > 0)
            def _():
                swap_copy(k, first).start()

        @pl.when((parity == 1) & (pair < pairs - 1))
        def _():
            early_rows()

    ready = jnp.where(pair == pairs - 1, blocks, jnp.minimum(pair, blocks - 1))

    @pl.loop(0, blocks + 1)
    def _(turn):
        @pl.when(turn == ready)
        def _():
            exchange()

        @pl.when(turn < blocks)
        def _():
            intra(turn)

    @pl.when(pair > 0)
    def _():
        for k in range(half):
            swap_copy(k, other).wait_recv()

    @pl.when(parity == 1)
    def _():
        for k in range(half):
            state_copy(other + k).wait_recv()
        for k in range(pieces):
            value = row_first[k, 0:1] * enter_in[k].astype(f32) + pair_state[k].astype(f32)
            entering[:, k * LANES : (k + 1) * LANES] = value.astype(bf16)

    @pl.when(parity == 0)
    def _():
        for k in range(pieces):
            entering[:, k * LANES : (k + 1) * LANES] = enter_in[k]

    gain = gain_ref[...].reshape(1, width)
    loads[1].wait()
    loads[2].wait()

    def near_copies(block):
        return [
            remote(one_out.at[block, 0], one_in.at[block, 0], one_send.at[block, 0], one_recv.at[block, 0], {"head": near}),
            remote(sq_out.at[block], sq_in.at[block], one_send.at[block, 1], one_recv.at[block, 1], {"head": near}),
            remote(one_out.at[block, 1], one_in.at[block, 1], one_send.at[block, 2], one_recv.at[block, 2], {"head": near}),
        ]

    def far_copies(block):
        return [
            remote(two_out.at[block], two_in.at[block], two_send.at[block, 0], two_recv.at[block, 0], {"head": far}),
            remote(sq_mid.at[block], sq_far.at[block], two_send.at[block, 1], two_recv.at[block, 1], {"head": far}),
        ]

    def product(index):
        at = pl.multiple_of(index * tile, LANES)
        return jnp.dot(unit[...], w_own[:, pl.ds(at, tile)], preferred_element_type=f32)

    @pl.loop(0, blocks)
    def _(block):
        start = pl.multiple_of(block * Q, Q)
        rows = pl.ds(start, Q)
        total = jnp.zeros((Q, LANES), f32)
        for col in range(0, width, CHUNK):
            cols = slice(col, col + CHUNK)
            wide = dot_t(fac2[block], spread_ref[:, cols])
            outer = jnp.dot(c_own[rows, :], entering[:, cols], preferred_element_type=f32)
            mixed = base[rows, cols] + wide * outer
            gated = mixed * silu(z_own[rows, cols].astype(f32))
            square = gated * gated
            for part in range(0, CHUNK, LANES):
                total = total + square[:, part : part + LANES]
            unit[:, cols] = (gated * gain[:, cols]).astype(bf16)
        sq_out[block] = lax.dot_general(
            jnp.ones((8, LANES), f32), total, (((1,), (1,)), ((), ())),
            precision=lax.Precision.HIGHEST, preferred_element_type=f32,
        )
        copies = near_copies(block)
        one_out[block, 0] = product(near_far).astype(bf16)
        copies[0].start()
        copies[1].start()
        two = product(far)
        copies[0].wait_recv()
        two_out[block] = (two + one_in[block, 0].astype(f32)).astype(bf16)
        copies[1].wait_recv()
        sq_mid[block] = sq_out[block] + sq_in[block]
        for copy in far_copies(block):
            copy.start()
        one_out[block, 1] = product(near).astype(bf16)
        copies[2].start()
        kept[block] = product(own)

    @pl.loop(0, blocks)
    def _(block):
        start = pl.multiple_of(block * Q, Q)
        near_copies(block)[2].wait_recv()
        for copy in far_copies(block):
            copy.wait_recv()
        squares = sq_mid[block] + sq_far[block]
        column = lax.dot_general(
            squares, jnp.full((8, LANES), 0.125, f32), (((0,), (0,)), ((), ())),
            precision=lax.Precision.HIGHEST, preferred_element_type=f32,
        )
        scale = lax.rsqrt(column / channels + norm_floor)[:, 0:1]
        out_ref[pl.ds(start, Q), :] = ((kept[block] + one_in[block, 1].astype(f32) + two_in[block].astype(f32)) * scale).astype(bf16)

    @pl.loop(0, blocks)
    def _(block):
        for copy in near_copies(block) + far_copies(block):
            copy.wait_send()

    @pl.when(me < shards - 1)
    def _():
        for copy in halo:
            copy.wait_send()

    give_log.wait_send()
    for k in range(half):
        state_copy(other + k).wait_send()

        @pl.when(parity == 0)
        def _():
            state_copy(first + k).wait_send()

    for k in range(half):
        @pl.when(pair > 0)
        def _():
            swap_copy(k, first).wait_send()

        @pl.when(pair < pairs - 1)
        def _():
            chain_copy(k).wait_send()


def local(shards, channels, x_raw, bc_raw, z_gate, dt_raw, a_log, d_skip, conv_x, conv_bc, norm_gain, w_out):
    length, width = x_raw.shape
    heads = a_log.shape[0]
    blocks = length // Q
    depth = w_out.shape[1]
    tile = depth // lax.axis_size("head")
    pieces = width // LANES
    half = pieces // 2
    spread = np.zeros((2 * SLOT, width), np.float32)
    for head in range(heads):
        spread[head, head * P_SIZE : (head + 1) * P_SIZE] = 1.0
        spread[SLOT + head, head * P_SIZE : (head + 1) * P_SIZE] = 1.0
    spread = jnp.asarray(spread, jnp.bfloat16)
    tri = jnp.asarray(np.triu(np.ones((Q, Q), np.float32)), jnp.bfloat16)
    f32, bf16 = jnp.float32, jnp.bfloat16
    anywhere = pl.BlockSpec(memory_space=pl.ANY)
    inside = pl.BlockSpec(memory_space=pltpu.VMEM)
    scalars = pl.BlockSpec(memory_space=pltpu.SMEM)
    vmem = pltpu.VMEM
    dma = pltpu.SemaphoreType.DMA
    return pl.pallas_call(
        functools.partial(layer_kernel, heads, width, length, depth, channels, shards),
        in_specs=[anywhere] * 4 + [inside] * 2 + [scalars] * 2 + [inside] * 5,
        out_specs=inside,
        out_shape=jax.ShapeDtypeStruct((length, tile), bf16),
        scratch_shapes=[
            vmem((length, width), bf16),
            vmem((length, width), bf16),
            vmem((width, depth), bf16),
            vmem((RIM, width), bf16),
            vmem((RIM, 2 * N), bf16),
            vmem((RIM + length, LANES), f32),
            vmem((RIM + length, 2 * N), f32),
            vmem((blocks, 2 * SLOT, 2 * Q + LANES), bf16),
            vmem((blocks, 2 * SLOT, Q), bf16),
            vmem((heads, LANES), f32),
            vmem((heads, LANES), f32),
            vmem((Q, Q), bf16),
            vmem((length, N), bf16),
            vmem((N, length), bf16),
            vmem((length, width), bf16),
            vmem((length, width), bf16),
            vmem((blocks, pieces, N, LANES), bf16),
            vmem((pieces, N, LANES), bf16),
            vmem((pieces, N, LANES), bf16),
            vmem((half, 8, LANES), f32),
            vmem((pieces, 8, LANES), f32),
            vmem((half, N, LANES), f32),
            vmem((length, width), f32),
            vmem((half, N, LANES), bf16),
            vmem((pieces, N, LANES), bf16),
            vmem((N, width), bf16),
            vmem((Q, width), bf16),
            vmem((blocks, 8, Q), f32),
            vmem((blocks, 8, Q), f32),
            vmem((blocks, 8, Q), f32),
            vmem((blocks, 8, Q), f32),
            vmem((blocks, 2, Q, tile), bf16),
            vmem((blocks, 2, Q, tile), bf16),
            vmem((blocks, Q, tile), f32),
            vmem((blocks, Q, tile), bf16),
            vmem((blocks, Q, tile), bf16),
            dma((3,)), dma((2,)), dma((2,)), dma((pieces,)), dma((pieces,)),
            dma((half,)), dma((half,)), dma((half,)), dma((half,)),
            dma((blocks, 3)), dma((blocks, 3)), dma((blocks, 2)), dma((blocks, 2)), dma((2,)),
        ],
        compiler_params=pltpu.CompilerParams(
            collective_id=0, has_side_effects=True, vmem_limit_bytes=63 << 20
        ),
    )(x_raw, z_gate, w_out, bc_raw, bc_raw, dt_raw, a_log, d_skip, conv_x, conv_bc, norm_gain, spread, tri)


def solution(mesh):
    in_specs = (
        P("seq", "head"),
        P("seq", None),
        P("seq", "head"),
        P("head", "seq"),
        P("head"),
        P("head"),
        P(None, "head"),
        P(),
        P("head"),
        P("head", None),
    )

    def whole(x_raw, *rest):
        body = functools.partial(local, mesh.shape["seq"], x_raw.shape[1])
        return jax.shard_map(
            body, mesh=mesh, in_specs=in_specs, out_specs=P("seq", "head"), check_vma=False
        )(x_raw, *rest)

    return whole
```
